32 devices in a mesh: row: 4 (over y, x), col: 8 (over z, core).
Axes of the slice: x: 2, y: 2, z: 4, core: 2. Of those that a mesh axis runs over, the one named last changes fastest.
Arguments:
- values: bfloat16 [4096, 4096], P('row', 'col'), may hold values from 0.0001296997 to 0.12988281
- tile_mask: int32 [32, 32], P('row', 'col'), may hold values 0 or 1
- keep_mask: int32 [32, 32], P('row', 'col'), may hold values 0 or 1
- thr_index: int32 [4096], P('col'), may hold values from 0 to 9
Outputs:
- expanded: bfloat16 [4096, 4096], P('row', 'col')
The draws below stay inside these ranges and needn't reach their ends.
All inputs are finite; a program needn't handle non-finite values. No bound on the sum of `tile_mask` or of `keep_mask` on one device may be relied on, other than what follows from the above.
Results may differ from the reference program's by a relative error of at most 0.0004.
Values may be sent and summed in bfloat16 or wider, within the bound.
A program may use at most 64 MiB of HBM per device.

```python
import math
import jax
import jax.numpy as jnp

TB = 128
NT = 32
ORDER = 4096


def touch_ends(values, stream_key, smallest, largest):
    spot = [jax.random.randint(jax.random.fold_in(stream_key, axis), (), 0, length) for axis, length in enumerate(values.shape)]
    longest = values.shape.index(max(values.shape))
    neighbour = spot[:longest] + [(spot[longest] + 1) % values.shape[longest]] + spot[longest + 1:]
    return values.at[tuple(spot)].set(smallest).at[tuple(neighbour)].set(largest)


def levels(stream_key, extent, shards, least, largest):
    level = 1.0
    for dim, shards_of in shards:
        draws = jax.random.uniform(jax.random.fold_in(jax.random.fold_in(stream_key, 6), dim), (shards_of,), jnp.float32, least / len(shards), largest / len(shards))
        level = level * jnp.repeat(jnp.exp(draws), extent[dim] // shards_of).reshape((-1,) + (1,) * (len(extent) - 1 - dim))
    return level


def setup_inputs(seed: int = 0) -> dict:
    seeds = jax.random.split(jax.random.key(seed), 5)
    values = jnp.clip(jnp.exp(math.log(0.12988281) - 6.909166 * jax.random.uniform(seeds[0], (ORDER, ORDER), jnp.float32) ** levels(seeds[0], (ORDER, ORDER), ((0, 4), (1, 8)), -0.2, 0.2)), 0.0001296997, 0.12988281).astype(jnp.bfloat16)
    tile_mask = touch_ends((jax.random.randint(seeds[1], (NT, NT), 0, 2) < 1).astype(jnp.int32), jax.random.fold_in(seeds[1], 1), 0, 1)
    keep_mask = touch_ends((jax.random.randint(seeds[2], (NT, NT), 0, 4) < 3).astype(jnp.int32), jax.random.fold_in(seeds[2], 1), 0, 1)
    thr_index = touch_ends(jax.random.randint(seeds[3], (ORDER,), 0, 10), jax.random.fold_in(seeds[3], 1), 0, 9).astype(jnp.int32)
    return {"values": values, "tile_mask": tile_mask, "keep_mask": keep_mask, "thr_index": thr_index}


def reference(values, tile_mask, keep_mask, thr_index):
    matrix = (values.reshape(NT, TB, NT, TB) * tile_mask[:, None, :, None].astype(jnp.bfloat16)).reshape(ORDER, ORDER)
    product = jnp.dot(matrix, matrix, preferred_element_type=jnp.float32)
    col_means = jnp.sum(product, axis=0) / ORDER
    thresholds = 0.125 * thr_index.astype(jnp.float32)
    kept_cells = jnp.broadcast_to(keep_mask[:, None, :, None].astype(jnp.float32), (NT, TB, NT, TB)).reshape(ORDER, ORDER)
    pruned = jnp.maximum(product - thresholds * col_means, 0.0) * kept_cells
    col_totals = jnp.sum(pruned, axis=0) / ORDER
    return (pruned / jnp.maximum(col_totals, 0.1)).astype(jnp.bfloat16)
```

```python
import functools

import jax
import jax.numpy as jnp
from jax import lax
from jax.experimental import pallas as pl
from jax.experimental.pallas import tpu as pltpu
from jax.sharding import PartitionSpec as P

TB = 128
CORES = 2
CHUNKS = 4


def snake(index, width):
    line, spot = index // width, index % width
    return line * width + spot + (line % 2) * (width - 1 - 2 * spot)


def kernel(
    row_dev, col_dev, width, chunks, order,
    v_ref, tile_ref, keep_ref, thr_ref, out_ref,
    row_panel, col_panel, acc, sums,
    line_send, line_recv, pair_send, pair_recv, ring_send, ring_recv, sum_send, sum_recv,
):
    rows, cols = v_ref.shape
    step_rows = rows // chunks
    chips = col_dev // CORES
    half = row_dev // 2
    me_row, me_col = lax.axis_index("row"), lax.axis_index("col")
    z, core = me_col // CORES, me_col % CORES
    pos = snake(me_row, width)

    def ring_device(offset):
        return snake((pos + offset + row_dev) % row_dev, width)

    barrier = pltpu.get_barrier_semaphore()
    pl.semaphore_signal(barrier, inc=1, device_id={"col": z * CORES + 1 - core})
    for d in range(1, row_dev):
        pl.semaphore_signal(barrier, inc=1, device_id={"row": (me_row + d) % row_dev})

    @pl.when(z > 0)
    def _():
        pl.semaphore_signal(barrier, inc=1, device_id={"col": me_col - CORES})

    @pl.when(z < chips - 1)
    def _():
        pl.semaphore_signal(barrier, inc=1, device_id={"col": me_col + CORES})

    for a in range(rows // TB):
        for b in range(cols // TB):
            r, c = slice(a * TB, (a + 1) * TB), slice(b * TB, (b + 1) * TB)
            scale = tile_ref[a, b].astype(jnp.float32)
            tile = (v_ref[r, c].astype(jnp.float32) * scale).astype(jnp.bfloat16)
            row_panel[me_col, r, c] = tile
            col_panel[pl.ds(pl.multiple_of(me_row * rows + a * TB, TB), TB), c] = tile

    pl.semaphore_wait(
        barrier, row_dev + (z > 0).astype(jnp.int32) + (z < chips - 1).astype(jnp.int32)
    )

    def row_part(block, q):
        return row_panel.at[block, pl.ds(q * step_rows, step_rows)]

    def line_copy(zi, q, to_right):
        part = row_part(zi * CORES + core, q)
        return pltpu.make_async_remote_copy(
            src_ref=part, dst_ref=part,
            send_sem=line_send.at[to_right, zi, q], recv_sem=line_recv.at[zi, q],
            device_id={"col": me_col + (CORES if to_right else -CORES)},
        )

    def pair_copy(zi, q, lane):
        part = row_part(zi * CORES + lane, q)
        return pltpu.make_async_remote_copy(
            src_ref=part, dst_ref=part,
            send_sem=pair_send.at[zi, q], recv_sem=pair_recv.at[zi, q],
            device_id={"col": z * CORES + 1 - core},
        )

    def ring_copy(owner, q, to_right):
        start = pl.multiple_of(owner * rows + q * step_rows, step_rows)
        part = col_panel.at[pl.ds(start, step_rows)]
        return pltpu.make_async_remote_copy(
            src_ref=part, dst_ref=part,
            send_sem=ring_send.at[to_right, owner, q], recv_sem=ring_recv.at[owner, q],
            device_id={"row": ring_device(1 if to_right else -1)},
        )

    def on_ring(d, q, to_right):
        if d < half:
            return True
        return d == half and (q < chunks // 2) == bool(to_right)

    def relay(zi, q, to_right, wait):
        if wait:
            line_copy(zi, q, to_right).wait_recv()
        go = (z < chips - 1) if to_right else (z > 0)

        @pl.when(go)
        def _():
            line_copy(zi, q, to_right).start()

    for q in range(chunks):
        for to_right in (1, 0):
            relay(z, q, to_right, False)
            if on_ring(1, q, to_right):
                ring_copy(me_row, q, to_right).start()
        pair_copy(z, q, core).start()

    def step(t, q):
        for to_right in (1, 0):
            valid = (z >= t) if to_right else (z + t < chips)
            zi = z - t if to_right else z + t
            if t < chips:
                @pl.when(valid)
                def _():
                    relay(zi, q, to_right, True)
                    pair_copy(zi, q, core).start()
            if on_ring(t, q, to_right):
                owner = ring_device(-t if to_right else t)
                ring_copy(owner, q, to_right).wait_recv()
                if on_ring(t + 1, q, to_right):
                    ring_copy(owner, q, to_right).start()

    def compute(zi, q, first=False):
        spot = pl.ds(pl.multiple_of(q * step_rows, step_rows), step_rows)
        total = None
        for lane in range(CORES):
            block = zi * CORES + lane
            inner = pl.ds(pl.multiple_of(block * cols, cols), cols)
            term = jnp.dot(
                row_panel[block, spot], col_panel[inner], preferred_element_type=jnp.float32
            )
            total = term if total is None else total + term
        if first:
            acc[spot] = total
        else:
            acc[spot] += total

    def take(zi, q, first=False):
        pair_copy(zi, q, 1 - core).wait_recv()
        compute(zi, q, first)

    def sides(t):
        return ((z >= t, z - t), (z + t < chips, z + t))

    def bulk(upto):
        @pl.loop(0, chunks)
        def _(q):
            take(z, q, True)
            for t in range(1, min(upto, chips - 1) + 1):
                for valid, zi in sides(t):
                    @pl.when(valid)
                    def _():
                        take(zi, q)

    if half == 0:
        bulk(0)
    for t in range(1, max(chips - 1, half) + 1):
        for q in range(chunks):
            step(t, q)
            if t > half:
                for valid, zi in sides(t):
                    @pl.when(valid)
                    def _():
                        take(zi, q)
        if t == half:
            bulk(t)

    def all_sum(phase, part):
        sums[phase, 0] = part

        def sum_copy(d):
            return pltpu.make_async_remote_copy(
                src_ref=sums.at[phase, 0], dst_ref=sums.at[phase, d],
                send_sem=sum_send.at[phase, d], recv_sem=sum_recv.at[phase, d],
                device_id={"row": (me_row + d) % row_dev},
            )

        for d in range(1, row_dev):
            sum_copy(d).start()
        total = part
        for d in range(1, row_dev):
            sum_copy(d).wait()
            total = total + sums[phase, d]
        return total

    cut = (
        0.125 * thr_ref[...].astype(jnp.float32)
        * (all_sum(0, jnp.sum(acc[...], axis=0, keepdims=True)) / order)
    )
    parts = []
    for b in range(cols // TB):
        c = slice(b * TB, (b + 1) * TB)
        part = jnp.zeros((1, TB), jnp.float32)
        for a in range(rows // TB):
            r = slice(a * TB, (a + 1) * TB)
            pruned = jnp.maximum(acc[r, c] - cut[:, c], 0.0) * keep_ref[a, b].astype(jnp.float32)
            acc[r, c] = pruned
            part += jnp.sum(pruned, axis=0, keepdims=True)
        parts.append(part)
    totals = all_sum(1, jnp.concatenate(parts, axis=1)) / order
    out_ref[...] = (acc[...] * (1.0 / jnp.maximum(totals, 0.1))).astype(jnp.bfloat16)

    for q in range(chunks):
        for zi in range(chips):
            pair_copy(zi, q, core).wait_send()

            @pl.when((z < chips - 1) & (z >= zi))
            def _():
                line_copy(zi, q, 1).wait_send()

            @pl.when((z > 0) & (z <= zi))
            def _():
                line_copy(zi, q, 0).wait_send()
        for d in range(0, half):
            for to_right in (1, 0):
                if on_ring(d + 1, q, to_right):
                    owner = ring_device(-d if to_right else d)
                    ring_copy(owner, q, to_right).wait_send()


def on_device(values, tile_mask, keep_mask, thr_index, *, row_dev, col_dev):
    rows, cols = values.shape
    width = max(w for w in range(1, row_dev + 1) if row_dev % w == 0 and w * w <= row_dev)
    chips = col_dev // CORES
    dma = pltpu.SemaphoreType.DMA
    return pl.pallas_call(
        functools.partial(kernel, row_dev, col_dev, width, CHUNKS, rows * row_dev),
        out_shape=jax.ShapeDtypeStruct((rows, cols), jnp.bfloat16),
        in_specs=[
            pl.BlockSpec(memory_space=pltpu.VMEM),
            pl.BlockSpec(memory_space=pltpu.SMEM),
            pl.BlockSpec(memory_space=pltpu.SMEM),
            pl.BlockSpec(memory_space=pltpu.VMEM),
        ],
        out_specs=pl.BlockSpec(memory_space=pltpu.VMEM),
        scratch_shapes=[
            pltpu.VMEM((col_dev, rows, cols), jnp.bfloat16),
            pltpu.VMEM((row_dev * rows, cols), jnp.bfloat16),
            pltpu.VMEM((rows, cols), jnp.float32),
            pltpu.VMEM((2, row_dev, 1, cols), jnp.float32),
            dma((2, chips, CHUNKS)),
            dma((chips, CHUNKS)),
            dma((chips, CHUNKS)),
            dma((chips, CHUNKS)),
            dma((2, row_dev, CHUNKS)),
            dma((row_dev, CHUNKS)),
            dma((2, row_dev)),
            dma((2, row_dev)),
        ],
        compiler_params=pltpu.CompilerParams(
            collective_id=0, has_side_effects=True, vmem_limit_bytes=60 * 1024 * 1024
        ),
    )(values, tile_mask, keep_mask, thr_index.reshape(1, cols))


def solution(mesh):
    return jax.shard_map(
        functools.partial(on_device, row_dev=mesh.shape["row"], col_dev=mesh.shape["col"]),
        mesh=mesh,
        in_specs=(P("row", "col"), P("row", "col"), P("row", "col"), P("col")),
        out_specs=P("row", "col"),
        check_vma=False,
    )
```

```python
import functools

import jax
import jax.numpy as jnp
from jax import lax
from jax.experimental import pallas as pl
from jax.experimental.pallas import tpu as pltpu
from jax.sharding import PartitionSpec as P

TB = 128
CORES = 2
CHUNKS = 8


def snake(index, width):
    line, spot = index // width, index % width
    return line * width + spot + (line % 2) * (width - 1 - 2 * spot)


def kernel(
    row_dev, col_dev, width, chunks, order,
    v_ref, tile_ref, keep_ref, thr_ref, pruned_ref, totals_ref,
    row_panel, col_panel, acc, sums, stats,
    line_send, line_recv, pair_send, pair_recv, ring_send, ring_recv,
    sum_send, sum_recv, stat_send, stat_recv, out_sem,
):
    rows, cols = v_ref.shape
    step_rows = rows // chunks
    chips = col_dev // CORES
    half = row_dev // 2
    me_row, me_col = lax.axis_index("row"), lax.axis_index("col")
    z, core = me_col // CORES, me_col % CORES
    pos = snake(me_row, width)

    def ring_device(offset):
        return snake((pos + offset + row_dev) % row_dev, width)

    barrier = pltpu.get_barrier_semaphore()
    for d in range(1, row_dev):
        pl.semaphore_signal(barrier, inc=1, device_id={"row": (me_row + d) % row_dev})
    for d in range(1, col_dev):
        pl.semaphore_signal(barrier, inc=1, device_id={"col": (me_col + d) % col_dev})

    stored = tile_ref[...].astype(jnp.float32)
    kept = keep_ref[...].astype(jnp.float32)
    for a in range(rows // TB):
        for b in range(cols // TB):
            r, c = slice(a * TB, (a + 1) * TB), slice(b * TB, (b + 1) * TB)
            scale = jnp.broadcast_to(stored[b : b + 1, a : a + 1], (TB, TB))
            tile = (v_ref[r, c].astype(jnp.float32) * scale).astype(jnp.bfloat16)
            row_panel[me_col, r, c] = tile
            col_panel[pl.ds(pl.multiple_of(me_row * rows + a * TB, TB), TB), c] = tile

    pl.semaphore_wait(barrier, row_dev + col_dev - 2)

    def row_part(block, q):
        return row_panel.at[block, pl.ds(q * step_rows, step_rows)]

    def line_copy(zi, q, to_right):
        part = row_part(zi * CORES + core, q)
        return pltpu.make_async_remote_copy(
            src_ref=part, dst_ref=part,
            send_sem=line_send.at[to_right, zi, q], recv_sem=line_recv.at[zi, q],
            device_id={"col": me_col + (CORES if to_right else -CORES)},
        )

    def pair_copy(zi, q, lane):
        part = row_part(zi * CORES + lane, q)
        return pltpu.make_async_remote_copy(
            src_ref=part, dst_ref=part,
            send_sem=pair_send.at[zi, q], recv_sem=pair_recv.at[zi, q],
            device_id={"col": z * CORES + 1 - core},
        )

    def ring_copy(owner, q, to_right):
        start = pl.multiple_of(owner * rows + q * step_rows, step_rows)
        part = col_panel.at[pl.ds(start, step_rows)]
        return pltpu.make_async_remote_copy(
            src_ref=part, dst_ref=part,
            send_sem=ring_send.at[to_right, owner, q], recv_sem=ring_recv.at[owner, q],
            device_id={"row": ring_device(1 if to_right else -1)},
        )

    def on_ring(d, q, to_right):
        if d < half:
            return True
        return d == half and (q < chunks // 2) == bool(to_right)

    def relay(zi, q, to_right, wait):
        if wait:
            line_copy(zi, q, to_right).wait_recv()
        go = (z < chips - 1) if to_right else (z > 0)

        @pl.when(go)
        def _():
            line_copy(zi, q, to_right).start()

    for q in range(chunks):
        for to_right in (1, 0):
            relay(z, q, to_right, False)
            if on_ring(1, q, to_right):
                ring_copy(me_row, q, to_right).start()
        pair_copy(z, q, core).start()

    def line_step(t, q):
        for to_right in (1, 0):
            valid = (z >= t) if to_right else (z + t < chips)
            zi = z - t if to_right else z + t
            if t < chips:
                @pl.when(valid)
                def _():
                    relay(zi, q, to_right, True)
                    pair_copy(zi, q, core).start()

    def ring_step(t, q):
        for to_right in (1, 0):
            if on_ring(t, q, to_right):
                owner = ring_device(-t if to_right else t)
                ring_copy(owner, q, to_right).wait_recv()
                if on_ring(t + 1, q, to_right):
                    ring_copy(owner, q, to_right).start()

    def stat_copy(d):
        return pltpu.make_async_remote_copy(
            src_ref=stats.at[0], dst_ref=stats.at[d],
            send_sem=stat_send.at[d], recv_sem=stat_recv.at[d],
            device_id={"col": (me_col + d) % col_dev},
        )

    def send_stats():
        total = jnp.zeros((1, cols), jnp.float32)
        for i in range(row_dev):
            block = col_panel[i * rows : (i + 1) * rows].astype(jnp.float32)
            total += jnp.sum(block, axis=0, keepdims=True)
        stats[0] = total
        for d in range(1, col_dev):
            stat_copy(d).start()

    def product_sums():
        total = jnp.zeros((1, cols), jnp.float32)
        for d in range(col_dev):
            if d:
                stat_copy(d).wait()
            block = (me_col - d + col_dev) % col_dev
            inner = pl.ds(pl.multiple_of(block * cols, cols), cols)
            rest, terms = stats[d], []
            for _ in range(3):
                term = rest.astype(jnp.bfloat16).astype(jnp.float32)
                rest = rest - term
                terms.append(jnp.broadcast_to(term, (8, cols)))
            spread = jnp.dot(
                jnp.concatenate(terms, axis=0).astype(jnp.bfloat16), col_panel[inner],
                preferred_element_type=jnp.float32,
            )
            total += spread[16:17] + spread[8:9] + spread[0:1]
        return total

    def compute(zi, q, first=False):
        spot = pl.ds(pl.multiple_of(q * step_rows, step_rows), step_rows)
        total = None
        for lane in range(CORES):
            block = zi * CORES + lane
            inner = pl.ds(pl.multiple_of(block * cols, cols), cols)
            term = jnp.dot(
                row_panel[block, spot], col_panel[inner], preferred_element_type=jnp.float32
            )
            total = term if total is None else total + term
        if first:
            acc[spot] = total
        else:
            acc[spot] += total

    def take(zi, q, first=False):
        pair_copy(zi, q, 1 - core).wait_recv()
        compute(zi, q, first)

    def sides(t):
        return ((z >= t, z - t), (z + t < chips, z + t))

    def bulk(upto):
        @pl.loop(0, chunks)
        def _(q):
            take(z, q, True)
            for t in range(1, min(upto, chips - 1) + 1):
                for valid, zi in sides(t):
                    @pl.when(valid)
                    def _():
                        take(zi, q)

    def out_copy(q):
        spot = pl.ds(q * step_rows, step_rows)
        return pltpu.make_async_copy(acc.at[spot], pruned_ref.at[spot], out_sem.at[q])

    def prune(q, cut):
        parts = []
        for b in range(cols // TB):
            c = slice(b * TB, (b + 1) * TB)
            part = jnp.zeros((1, TB), jnp.float32)
            for lo in range(q * step_rows, (q + 1) * step_rows, min(step_rows, TB)):
                r = slice(lo, lo + min(step_rows, TB))
                keep = jnp.broadcast_to(kept[b : b + 1, lo // TB : lo // TB + 1], (r.stop - lo, TB))
                pruned = jnp.maximum(acc[r, c] - cut[:, c], 0.0) * keep
                acc[r, c] = pruned
                part += jnp.sum(pruned, axis=0, keepdims=True)
            parts.append(part)
        return jnp.concatenate(parts, axis=1)

    def cuts():
        return 0.125 * thr_ref[...].astype(jnp.float32) * (product_sums() / order)

    part = jnp.zeros((1, cols), jnp.float32)
    last = max(chips - 1, half)
    if half == 0:
        send_stats()
        bulk(0)
    for t in range(1, last + 1):
        if t == half:
            for q in range(chunks):
                ring_step(t, q)
            send_stats()
            for q in range(chunks):
                line_step(t, q)
            bulk(t)
        else:
            if t == last and t > half:
                cut = cuts()
            for q in range(chunks):
                line_step(t, q)
                if t < half:
                    ring_step(t, q)
                else:
                    for valid, zi in sides(t):
                        @pl.when(valid)
                        def _():
                            take(zi, q)
                    if t == last:
                        part += prune(q, cut)
                        out_copy(q).start()
    if last <= half:
        cut = cuts()
        for q in range(chunks):
            part += prune(q, cut)
            out_copy(q).start()

    sums[0] = part

    def sum_copy(d):
        return pltpu.make_async_remote_copy(
            src_ref=sums.at[0], dst_ref=sums.at[d],
            send_sem=sum_send.at[d], recv_sem=sum_recv.at[d],
            device_id={"row": (me_row + d) % row_dev},
        )

    for d in range(1, row_dev):
        sum_copy(d).start()
    for d in range(1, row_dev):
        sum_copy(d).wait()
        part += sums[d]
    totals_ref[...] = 1.0 / jnp.maximum(part / order, 0.1)

    for q in range(chunks):
        out_copy(q).wait()

    for q in range(chunks):
        for zi in range(chips):
            pair_copy(zi, q, core).wait_send()

            @pl.when((z < chips - 1) & (z >= zi))
            def _():
                line_copy(zi, q, 1).wait_send()

            @pl.when((z > 0) & (z <= zi))
            def _():
                line_copy(zi, q, 0).wait_send()
        for d in range(0, half):
            for to_right in (1, 0):
                if on_ring(d + 1, q, to_right):
                    owner = ring_device(-d if to_right else d)
                    ring_copy(owner, q, to_right).wait_send()


def on_device(values, tile_mask, keep_mask, thr_index, *, row_dev, col_dev):
    rows, cols = values.shape
    width = max(w for w in range(1, row_dev + 1) if row_dev % w == 0 and w * w <= row_dev)
    chips = col_dev // CORES
    dma = pltpu.SemaphoreType.DMA
    vmem = pl.BlockSpec(memory_space=pltpu.VMEM)
    pruned, scale = pl.pallas_call(
        functools.partial(kernel, row_dev, col_dev, width, CHUNKS, rows * row_dev),
        out_shape=(
            jax.ShapeDtypeStruct((rows, cols), jnp.float32),
            jax.ShapeDtypeStruct((1, cols), jnp.float32),
        ),
        in_specs=[vmem] * 4,
        out_specs=(pl.BlockSpec(memory_space=pl.ANY), vmem),
        scratch_shapes=[
            pltpu.VMEM((col_dev, rows, cols), jnp.bfloat16),
            pltpu.VMEM((row_dev * rows, cols), jnp.bfloat16),
            pltpu.VMEM((rows, cols), jnp.float32),
            pltpu.VMEM((row_dev, 1, cols), jnp.float32),
            pltpu.VMEM((col_dev, 1, cols), jnp.float32),
            dma((2, chips, CHUNKS)),
            dma((chips, CHUNKS)),
            dma((chips, CHUNKS)),
            dma((chips, CHUNKS)),
            dma((2, row_dev, CHUNKS)),
            dma((row_dev, CHUNKS)),
            dma((row_dev,)),
            dma((row_dev,)),
            dma((col_dev,)),
            dma((col_dev,)),
            dma((CHUNKS,)),
        ],
        compiler_params=pltpu.CompilerParams(
            collective_id=0, has_side_effects=True, vmem_limit_bytes=60 * 1024 * 1024
        ),
    )(values, tile_mask.T, keep_mask.T, thr_index.reshape(1, cols))
    return (pruned * scale).astype(jnp.bfloat16)


def solution(mesh):
    return jax.shard_map(
        functools.partial(on_device, row_dev=mesh.shape["row"], col_dev=mesh.shape["col"]),
        mesh=mesh,
        in_specs=(P("row", "col"), P("row", "col"), P("row", "col"), P("col")),
        out_specs=P("row", "col"),
        check_vma=False,
    )
```

```python
import functools

import jax
import jax.numpy as jnp
from jax import lax
from jax.experimental import pallas as pl
from jax.experimental.pallas import tpu as pltpu
from jax.sharding import PartitionSpec as P

TB = 128
CORES = 2
CHUNKS = 8


def snake(index, width):
    line, spot = index // width, index % width
    return line * width + spot + (line % 2) * (width - 1 - 2 * spot)


def kernel(
    row_dev, col_dev, width, chunks, order,
    v_ref, tile_ref, keep_ref, thr_ref, pruned_ref, totals_ref,
    row_panel, col_panel, acc, sums, stats,
    line_send, line_recv, pair_send, pair_recv, ring_send, ring_recv,
    sum_send, sum_recv, stat_send, stat_recv, out_sem, loaded, load_sem, token,
):
    rows, cols = v_ref.shape
    step_rows = rows // chunks
    chips = col_dev // CORES
    half = row_dev // 2
    me_row, me_col = lax.axis_index("row"), lax.axis_index("col")
    z, core = me_col // CORES, me_col % CORES
    pos = snake(me_row, width)

    def ring_device(offset):
        return snake((pos + offset + row_dev) % row_dev, width)

    barrier = pltpu.get_barrier_semaphore()
    pl.semaphore_signal(barrier, inc=1, device_id={"col": z * CORES + 1 - core})
    peers = 1 + (z > 0).astype(jnp.int32) + (z < chips - 1).astype(jnp.int32)
    for offset in ((1, -1) if row_dev > 2 else (1,) * half):
        pl.semaphore_signal(barrier, inc=1, device_id={"row": ring_device(offset)})
        peers += 1

    @pl.when(z > 0)
    def _():
        pl.semaphore_signal(barrier, inc=1, device_id={"col": me_col - CORES})

    @pl.when(z < chips - 1)
    def _():
        pl.semaphore_signal(barrier, inc=1, device_id={"col": me_col + CORES})

    def load(q):
        spot = pl.ds(q * step_rows, step_rows)
        return pltpu.make_async_copy(v_ref.at[spot], loaded.at[spot], load_sem.at[q])

    for q in range(chunks):
        load(q).start()

    stored = tile_ref[...].astype(jnp.float32)
    kept = keep_ref[...].astype(jnp.float32)
    height = min(step_rows, TB)
    for lo in range(0, rows, height):
        if lo % step_rows == 0:
            load(lo // step_rows).wait()
        for b in range(cols // TB):
            r, c = slice(lo, lo + height), slice(b * TB, (b + 1) * TB)
            scale = jnp.broadcast_to(stored[b : b + 1, lo // TB : lo // TB + 1], (height, TB))
            tile = (loaded[r, c].astype(jnp.float32) * scale).astype(jnp.bfloat16)
            row_panel[me_col, r, c] = tile
            col_panel[pl.ds(pl.multiple_of(me_row * rows + lo, height), height), c] = tile

    pl.semaphore_wait(barrier, peers)

    def row_part(block, q):
        return row_panel.at[block, pl.ds(q * step_rows, step_rows)]

    def line_copy(zi, q, to_right):
        part = row_part(zi * CORES + core, q)
        return pltpu.make_async_remote_copy(
            src_ref=part, dst_ref=part,
            send_sem=line_send.at[to_right, zi, q], recv_sem=line_recv.at[zi, q],
            device_id={"col": me_col + (CORES if to_right else -CORES)},
        )

    def pair_copy(zi, q, lane):
        part = row_part(zi * CORES + lane, q)
        return pltpu.make_async_remote_copy(
            src_ref=part, dst_ref=part,
            send_sem=pair_send.at[zi, q], recv_sem=pair_recv.at[zi, q],
            device_id={"col": z * CORES + 1 - core},
        )

    def ring_copy(owner, q, to_right):
        start = pl.multiple_of(owner * rows + q * step_rows, step_rows)
        part = col_panel.at[pl.ds(start, step_rows)]
        return pltpu.make_async_remote_copy(
            src_ref=part, dst_ref=part,
            send_sem=ring_send.at[to_right, owner, q], recv_sem=ring_recv.at[owner, q],
            device_id={"row": ring_device(1 if to_right else -1)},
        )

    def on_ring(d, q, to_right):
        if d < half:
            return True
        return d == half and (q < chunks // 2) == bool(to_right)

    def relay(zi, q, to_right, wait):
        if wait:
            line_copy(zi, q, to_right).wait_recv()
        go = (z < chips - 1) if to_right else (z > 0)

        @pl.when(go)
        def _():
            line_copy(zi, q, to_right).start()

    for q in range(chunks):
        for to_right in (1, 0):
            relay(z, q, to_right, False)
            if on_ring(1, q, to_right):
                ring_copy(me_row, q, to_right).start()
        pair_copy(z, q, core).start()

    for to_right in (1, 0):
        first, end = (0, chips - 1) if to_right else (chips - 1, 0)

        @pl.when(z != first)
        def _():
            pl.semaphore_wait(token.at[to_right], 1)

        @pl.when(z != end)
        def _():
            pl.semaphore_signal(
                token.at[to_right], inc=1,
                device_id={"col": me_col + (CORES if to_right else -CORES)},
            )

    def line_step(t, q):
        for to_right in (1, 0):
            valid = (z >= t) if to_right else (z + t < chips)
            zi = z - t if to_right else z + t
            if t < chips:
                @pl.when(valid)
                def _():
                    relay(zi, q, to_right, True)
                    pair_copy(zi, q, core).start()

    def ring_step(t, q):
        for to_right in (1, 0):
            if on_ring(t, q, to_right):
                owner = ring_device(-t if to_right else t)
                ring_copy(owner, q, to_right).wait_recv()
                if on_ring(t + 1, q, to_right):
                    ring_copy(owner, q, to_right).start()

    def stat_copy(d):
        return pltpu.make_async_remote_copy(
            src_ref=stats.at[0], dst_ref=stats.at[d],
            send_sem=stat_send.at[d], recv_sem=stat_recv.at[d],
            device_id={"col": (me_col + d) % col_dev},
        )

    def send_stats():
        total = jnp.zeros((1, cols), jnp.float32)
        for i in range(row_dev):
            block = col_panel[i * rows : (i + 1) * rows].astype(jnp.float32)
            total += jnp.sum(block, axis=0, keepdims=True)
        stats[0] = total
        for d in range(1, col_dev):
            stat_copy(d).start()

    def product_sums():
        total = jnp.zeros((1, cols), jnp.float32)
        for d in range(col_dev):
            if d:
                stat_copy(d).wait()
            block = (me_col - d + col_dev) % col_dev
            inner = pl.ds(pl.multiple_of(block * cols, cols), cols)
            rest, terms = stats[d], []
            for _ in range(3):
                term = rest.astype(jnp.bfloat16).astype(jnp.float32)
                rest = rest - term
                terms.append(jnp.broadcast_to(term, (8, cols)))
            spread = jnp.dot(
                jnp.concatenate(terms, axis=0).astype(jnp.bfloat16), col_panel[inner],
                preferred_element_type=jnp.float32,
            )
            total += spread[16:17] + spread[8:9] + spread[0:1]
        return total

    def compute(zi, q, first=False):
        spot = pl.ds(pl.multiple_of(q * step_rows, step_rows), step_rows)
        total = None
        for lane in range(CORES):
            block = zi * CORES + lane
            inner = pl.ds(pl.multiple_of(block * cols, cols), cols)
            term = jnp.dot(
                row_panel[block, spot], col_panel[inner], preferred_element_type=jnp.float32
            )
            total = term if total is None else total + term
        if first:
            acc[spot] = total
        else:
            acc[spot] += total

    def take(zi, q, first=False):
        pair_copy(zi, q, 1 - core).wait_recv()
        compute(zi, q, first)

    def sides(t):
        return ((z >= t, z - t), (z + t < chips, z + t))

    def bulk(upto):
        @pl.loop(0, chunks)
        def _(q):
            take(z, q, True)
            for t in range(1, min(upto, chips - 1) + 1):
                for valid, zi in sides(t):
                    @pl.when(valid)
                    def _():
                        take(zi, q)

    def out_copy(q):
        spot = pl.ds(q * step_rows, step_rows)
        return pltpu.make_async_copy(acc.at[spot], pruned_ref.at[spot], out_sem.at[q])

    def prune(q, cut):
        parts = []
        for b in range(cols // TB):
            c = slice(b * TB, (b + 1) * TB)
            part = jnp.zeros((1, TB), jnp.float32)
            for lo in range(q * step_rows, (q + 1) * step_rows, min(step_rows, TB)):
                r = slice(lo, lo + min(step_rows, TB))
                keep = jnp.broadcast_to(kept[b : b + 1, lo // TB : lo // TB + 1], (r.stop - lo, TB))
                pruned = jnp.maximum(acc[r, c] - cut[:, c], 0.0) * keep
                acc[r, c] = pruned
                part += jnp.sum(pruned, axis=0, keepdims=True)
            parts.append(part)
        return jnp.concatenate(parts, axis=1)

    def cuts():
        return 0.125 * thr_ref[...].astype(jnp.float32) * (product_sums() / order)

    part = jnp.zeros((1, cols), jnp.float32)
    last = max(chips - 1, half)
    if half == 0:
        send_stats()
        bulk(0)
    for t in range(1, last + 1):
        if t == half:
            for q in range(chunks):
                ring_step(t, q)
            send_stats()
            for q in range(chunks):
                line_step(t, q)
            bulk(t)
        else:
            if t == last and t > half:
                cut = cuts()
            for q in range(chunks):
                line_step(t, q)
                if t < half:
                    ring_step(t, q)
                else:
                    for valid, zi in sides(t):
                        @pl.when(valid)
                        def _():
                            take(zi, q)
                    if t == last:
                        part += prune(q, cut)
                        out_copy(q).start()
    if last <= half:
        cut = cuts()
        for q in range(chunks):
            part += prune(q, cut)
            out_copy(q).start()

    sums[0] = part

    def sum_copy(d):
        return pltpu.make_async_remote_copy(
            src_ref=sums.at[0], dst_ref=sums.at[d],
            send_sem=sum_send.at[d], recv_sem=sum_recv.at[d],
            device_id={"row": (me_row + d) % row_dev},
        )

    for d in range(1, row_dev):
        sum_copy(d).start()
    for d in range(1, row_dev):
        sum_copy(d).wait()
        part += sums[d]
    totals_ref[...] = 1.0 / jnp.maximum(part / order, 0.1)

    for q in range(chunks):
        out_copy(q).wait()

    for q in range(chunks):
        for zi in range(chips):
            pair_copy(zi, q, core).wait_send()

            @pl.when((z < chips - 1) & (z >= zi))
            def _():
                line_copy(zi, q, 1).wait_send()

            @pl.when((z > 0) & (z <= zi))
            def _():
                line_copy(zi, q, 0).wait_send()
        for d in range(0, half):
            for to_right in (1, 0):
                if on_ring(d + 1, q, to_right):
                    owner = ring_device(-d if to_right else d)
                    ring_copy(owner, q, to_right).wait_send()


def on_device(values, tile_mask, keep_mask, thr_index, *, row_dev, col_dev):
    rows, cols = values.shape
    width = max(w for w in range(1, row_dev + 1) if row_dev % w == 0 and w * w <= row_dev)
    chips = col_dev // CORES
    dma = pltpu.SemaphoreType.DMA
    vmem = pl.BlockSpec(memory_space=pltpu.VMEM)
    pruned, scale = pl.pallas_call(
        functools.partial(kernel, row_dev, col_dev, width, CHUNKS, rows * row_dev),
        out_shape=(
            jax.ShapeDtypeStruct((rows, cols), jnp.float32),
            jax.ShapeDtypeStruct((1, cols), jnp.float32),
        ),
        in_specs=[pl.BlockSpec(memory_space=pl.ANY)] + [vmem] * 3,
        out_specs=(pl.BlockSpec(memory_space=pl.ANY), vmem),
        scratch_shapes=[
            pltpu.VMEM((col_dev, rows, cols), jnp.bfloat16),
            pltpu.VMEM((row_dev * rows, cols), jnp.bfloat16),
            pltpu.VMEM((rows, cols), jnp.float32),
            pltpu.VMEM((row_dev, 1, cols), jnp.float32),
            pltpu.VMEM((col_dev, 1, cols), jnp.float32),
            dma((2, chips, CHUNKS)),
            dma((chips, CHUNKS)),
            dma((chips, CHUNKS)),
            dma((chips, CHUNKS)),
            dma((2, row_dev, CHUNKS)),
            dma((row_dev, CHUNKS)),
            dma((row_dev,)),
            dma((row_dev,)),
            dma((col_dev,)),
            dma((col_dev,)),
            dma((CHUNKS,)),
            pltpu.VMEM((rows, cols), jnp.bfloat16),
            dma((CHUNKS,)),
            pltpu.SemaphoreType.REGULAR((2,)),
        ],
        compiler_params=pltpu.CompilerParams(
            collective_id=0, has_side_effects=True, vmem_limit_bytes=60 * 1024 * 1024
        ),
    )(values, tile_mask.T, keep_mask.T, thr_index.reshape(1, cols))
    return (pruned * scale).astype(jnp.bfloat16)


def solution(mesh):
    return jax.shard_map(
        functools.partial(on_device, row_dev=mesh.shape["row"], col_dev=mesh.shape["col"]),
        mesh=mesh,
        in_specs=(P("row", "col"), P("row", "col"), P("row", "col"), P("col")),
        out_specs=P("row", "col"),
        check_vma=False,
    )
```

```python
import functools

import jax
import jax.numpy as jnp
from jax import lax
from jax.experimental import pallas as pl
from jax.experimental.pallas import tpu as pltpu
from jax.sharding import PartitionSpec as P

TB = 128
CORES = 2
CHUNKS = 8


def snake(index, width):
    line, spot = index // width, index % width
    return line * width + spot + (line % 2) * (width - 1 - 2 * spot)


def kernel(
    row_dev, col_dev, width, chunks, order,
    v_ref, tile_ref, keep_ref, thr_ref, acc, totals_ref,
    row_panel, col_panel, sums, stats,
    line_send, line_recv, pair_send, pair_recv, ring_send, ring_recv,
    sum_send, sum_recv, stat_send, stat_recv, loaded, load_sem, token,
):
    rows, cols = v_ref.shape
    step_rows = rows // chunks
    chips = col_dev // CORES
    half = row_dev // 2
    me_row, me_col = lax.axis_index("row"), lax.axis_index("col")
    z, core = me_col // CORES, me_col % CORES
    pos = snake(me_row, width)

    def ring_device(offset):
        return snake((pos + offset + row_dev) % row_dev, width)

    barrier = pltpu.get_barrier_semaphore()
    pl.semaphore_signal(barrier, inc=1, device_id={"col": z * CORES + 1 - core})
    peers = 1 + (z > 0).astype(jnp.int32) + (z < chips - 1).astype(jnp.int32)
    for offset in ((1, -1) if row_dev > 2 else (1,) * half):
        pl.semaphore_signal(barrier, inc=1, device_id={"row": ring_device(offset)})
        peers += 1

    @pl.when(z > 0)
    def _():
        pl.semaphore_signal(barrier, inc=1, device_id={"col": me_col - CORES})

    @pl.when(z < chips - 1)
    def _():
        pl.semaphore_signal(barrier, inc=1, device_id={"col": me_col + CORES})

    def load(q):
        spot = pl.ds(q * step_rows, step_rows)
        return pltpu.make_async_copy(v_ref.at[spot], loaded.at[spot], load_sem.at[q])

    for q in range(chunks):
        load(q).start()

    stored = tile_ref[...].astype(jnp.float32)
    kept = keep_ref[...].astype(jnp.float32)
    height = min(step_rows, TB)
    for lo in range(0, rows, height):
        if lo % step_rows == 0:
            load(lo // step_rows).wait()
        for b in range(cols // TB):
            r, c = slice(lo, lo + height), slice(b * TB, (b + 1) * TB)
            scale = jnp.broadcast_to(stored[b : b + 1, lo // TB : lo // TB + 1], (height, TB))
            tile = (loaded[r, c].astype(jnp.float32) * scale).astype(jnp.bfloat16)
            row_panel[me_col, r, c] = tile
            col_panel[pl.ds(pl.multiple_of(me_row * rows + lo, height), height), c] = tile

    pl.semaphore_wait(barrier, peers)

    def row_part(block, q):
        return row_panel.at[block, pl.ds(q * step_rows, step_rows)]

    def line_copy(zi, q, to_right):
        part = row_part(zi * CORES + core, q)
        return pltpu.make_async_remote_copy(
            src_ref=part, dst_ref=part,
            send_sem=line_send.at[to_right, zi, q], recv_sem=line_recv.at[zi, q],
            device_id={"col": me_col + (CORES if to_right else -CORES)},
        )

    def pair_copy(zi, q, lane):
        part = row_part(zi * CORES + lane, q)
        return pltpu.make_async_remote_copy(
            src_ref=part, dst_ref=part,
            send_sem=pair_send.at[zi, q], recv_sem=pair_recv.at[zi, q],
            device_id={"col": z * CORES + 1 - core},
        )

    def ring_copy(owner, q, to_right):
        start = pl.multiple_of(owner * rows + q * step_rows, step_rows)
        part = col_panel.at[pl.ds(start, step_rows)]
        return pltpu.make_async_remote_copy(
            src_ref=part, dst_ref=part,
            send_sem=ring_send.at[to_right, owner, q], recv_sem=ring_recv.at[owner, q],
            device_id={"row": ring_device(1 if to_right else -1)},
        )

    def on_ring(d, q, to_right):
        if d < half:
            return True
        return d == half and (q < chunks // 2) == bool(to_right)

    def relay(zi, q, to_right, wait):
        if wait:
            line_copy(zi, q, to_right).wait_recv()
        go = (z < chips - 1) if to_right else (z > 0)

        @pl.when(go)
        def _():
            line_copy(zi, q, to_right).start()

    for q in range(chunks):
        for to_right in (1, 0):
            relay(z, q, to_right, False)
            if on_ring(1, q, to_right):
                ring_copy(me_row, q, to_right).start()
        pair_copy(z, q, core).start()

    for to_right in (1, 0):
        first, end = (0, chips - 1) if to_right else (chips - 1, 0)

        @pl.when(z != first)
        def _():
            pl.semaphore_wait(token.at[to_right], 1)

        @pl.when(z != end)
        def _():
            pl.semaphore_signal(
                token.at[to_right], inc=1,
                device_id={"col": me_col + (CORES if to_right else -CORES)},
            )

    def line_step(t, q):
        for to_right in (1, 0):
            valid = (z >= t) if to_right else (z + t < chips)
            zi = z - t if to_right else z + t
            if t < chips:
                @pl.when(valid)
                def _():
                    relay(zi, q, to_right, True)
                    pair_copy(zi, q, core).start()

    def ring_step(t, q):
        for to_right in (1, 0):
            if on_ring(t, q, to_right):
                owner = ring_device(-t if to_right else t)
                ring_copy(owner, q, to_right).wait_recv()
                if on_ring(t + 1, q, to_right):
                    ring_copy(owner, q, to_right).start()

    def stat_copy(d):
        return pltpu.make_async_remote_copy(
            src_ref=stats.at[0], dst_ref=stats.at[d],
            send_sem=stat_send.at[d], recv_sem=stat_recv.at[d],
            device_id={"col": (me_col + d) % col_dev},
        )

    def send_stats():
        total = jnp.zeros((1, cols), jnp.float32)
        for i in range(row_dev):
            block = col_panel[i * rows : (i + 1) * rows].astype(jnp.float32)
            total += jnp.sum(block, axis=0, keepdims=True)
        stats[0] = total
        for d in range(1, col_dev):
            stat_copy(d).start()

    def product_sums():
        total = jnp.zeros((1, cols), jnp.float32)
        for d in range(col_dev):
            if d:
                stat_copy(d).wait()
            block = (me_col - d + col_dev) % col_dev
            inner = pl.ds(pl.multiple_of(block * cols, cols), cols)
            rest, terms = stats[d], []
            for _ in range(3):
                term = rest.astype(jnp.bfloat16).astype(jnp.float32)
                rest = rest - term
                terms.append(jnp.broadcast_to(term, (8, cols)))
            spread = jnp.dot(
                jnp.concatenate(terms, axis=0).astype(jnp.bfloat16), col_panel[inner],
                preferred_element_type=jnp.float32,
            )
            total += spread[16:17] + spread[8:9] + spread[0:1]
        return total

    def compute(zi, q, first=False):
        spot = pl.ds(pl.multiple_of(q * step_rows, step_rows), step_rows)
        total = None
        for lane in range(CORES):
            block = zi * CORES + lane
            inner = pl.ds(pl.multiple_of(block * cols, cols), cols)
            term = jnp.dot(
                row_panel[block, spot], col_panel[inner], preferred_element_type=jnp.float32
            )
            total = term if total is None else total + term
        if first:
            acc[spot] = total
        else:
            acc[spot] += total

    def take(zi, q, first=False):
        pair_copy(zi, q, 1 - core).wait_recv()
        compute(zi, q, first)

    def sides(t):
        return ((z >= t, z - t), (z + t < chips, z + t))

    def bulk(upto):
        @pl.loop(0, chunks)
        def _(q):
            take(z, q, True)
            for t in range(1, min(upto, chips - 1) + 1):
                for valid, zi in sides(t):
                    @pl.when(valid)
                    def _():
                        take(zi, q)

    def prune(q, cut):
        parts = []
        for b in range(cols // TB):
            c = slice(b * TB, (b + 1) * TB)
            part = jnp.zeros((1, TB), jnp.float32)
            for lo in range(q * step_rows, (q + 1) * step_rows, min(step_rows, TB)):
                r = slice(lo, lo + min(step_rows, TB))
                keep = jnp.broadcast_to(kept[b : b + 1, lo // TB : lo // TB + 1], (r.stop - lo, TB))
                pruned = jnp.maximum(acc[r, c] - cut[:, c], 0.0) * keep
                acc[r, c] = pruned
                part += jnp.sum(pruned, axis=0, keepdims=True)
            parts.append(part)
        return jnp.concatenate(parts, axis=1)

    def cuts():
        return 0.125 * thr_ref[...].astype(jnp.float32) * (product_sums() / order)

    part = jnp.zeros((1, cols), jnp.float32)
    last = max(chips - 1, half)
    if half == 0:
        send_stats()
        bulk(0)
    for t in range(1, last + 1):
        if t == half:
            for q in range(chunks):
                ring_step(t, q)
            send_stats()
            for q in range(chunks):
                line_step(t, q)
            bulk(t)
        else:
            if t == last and t > half:
                cut = cuts()
            for q in range(chunks):
                line_step(t, q)
                if t < half:
                    ring_step(t, q)
                else:
                    for valid, zi in sides(t):
                        @pl.when(valid)
                        def _():
                            take(zi, q)
                    if t == last:
                        part += prune(q, cut)
    if last <= half:
        cut = cuts()
        for q in range(chunks):
            part += prune(q, cut)

    sums[0] = part

    def sum_copy(d):
        return pltpu.make_async_remote_copy(
            src_ref=sums.at[0], dst_ref=sums.at[d],
            send_sem=sum_send.at[d], recv_sem=sum_recv.at[d],
            device_id={"row": (me_row + d) % row_dev},
        )

    for d in range(1, row_dev):
        sum_copy(d).start()
    for d in range(1, row_dev):
        sum_copy(d).wait()
        part += sums[d]
    totals_ref[...] = 1.0 / jnp.maximum(part / order, 0.1)

    for q in range(chunks):
        for zi in range(chips):
            pair_copy(zi, q, core).wait_send()

            @pl.when((z < chips - 1) & (z >= zi))
            def _():
                line_copy(zi, q, 1).wait_send()

            @pl.when((z > 0) & (z <= zi))
            def _():
                line_copy(zi, q, 0).wait_send()
        for d in range(0, half):
            for to_right in (1, 0):
                if on_ring(d + 1, q, to_right):
                    owner = ring_device(-d if to_right else d)
                    ring_copy(owner, q, to_right).wait_send()


def on_device(values, tile_mask, keep_mask, thr_index, *, row_dev, col_dev):
    rows, cols = values.shape
    width = max(w for w in range(1, row_dev + 1) if row_dev % w == 0 and w * w <= row_dev)
    chips = col_dev // CORES
    dma = pltpu.SemaphoreType.DMA
    vmem = pl.BlockSpec(memory_space=pltpu.VMEM)
    pruned, scale = pl.pallas_call(
        functools.partial(kernel, row_dev, col_dev, width, CHUNKS, rows * row_dev),
        out_shape=(
            pltpu.VMEM((rows, cols), jnp.float32),
            jax.ShapeDtypeStruct((1, cols), jnp.float32),
        ),
        in_specs=[pl.BlockSpec(memory_space=pl.ANY)] + [vmem] * 3,
        out_specs=(vmem, vmem),
        scratch_shapes=[
            pltpu.VMEM((col_dev, rows, cols), jnp.bfloat16),
            pltpu.VMEM((row_dev * rows, cols), jnp.bfloat16),
            pltpu.VMEM((row_dev, 1, cols), jnp.float32),
            pltpu.VMEM((col_dev, 1, cols), jnp.float32),
            dma((2, chips, CHUNKS)),
            dma((chips, CHUNKS)),
            dma((chips, CHUNKS)),
            dma((chips, CHUNKS)),
            dma((2, row_dev, CHUNKS)),
            dma((row_dev, CHUNKS)),
            dma((row_dev,)),
            dma((row_dev,)),
            dma((col_dev,)),
            dma((col_dev,)),
            pltpu.VMEM((rows, cols), jnp.bfloat16),
            dma((CHUNKS,)),
            pltpu.SemaphoreType.REGULAR((2,)),
        ],
        compiler_params=pltpu.CompilerParams(
            collective_id=0, has_side_effects=True,
            vmem_limit_bytes=63 * 2**20 - 4 * rows * cols + 2**19,
        ),
    )(values, tile_mask.T, keep_mask.T, thr_index.reshape(1, cols))
    return (pruned * scale).astype(jnp.bfloat16)


def solution(mesh):
    return jax.shard_map(
        functools.partial(on_device, row_dev=mesh.shape["row"], col_dev=mesh.shape["col"]),
        mesh=mesh,
        in_specs=(P("row", "col"), P("row", "col"), P("row", "col"), P("col")),
        out_specs=P("row", "col"),
        check_vma=False,
    )
```

```python
import functools

import jax
import jax.numpy as jnp
from jax import lax
from jax.experimental import pallas as pl
from jax.experimental.pallas import tpu as pltpu
from jax.sharding import PartitionSpec as P

TB = 128
CORES = 2
CHUNKS = 16


def snake(index, width):
    line, spot = index // width, index % width
    return line * width + spot + (line % 2) * (width - 1 - 2 * spot)


def kernel(
    row_dev, col_dev, width, chunks, order,
    v_ref, tile_ref, keep_ref, thr_ref, acc, totals_ref,
    row_panel, col_panel, sums, stats,
    line_send, line_recv, pair_send, pair_recv, ring_send, ring_recv,
    sum_send, sum_recv, stat_send, stat_recv, loaded, load_sem, token,
):
    rows, cols = v_ref.shape
    step_rows = rows // chunks
    chips = col_dev // CORES
    half = row_dev // 2
    me_row, me_col = lax.axis_index("row"), lax.axis_index("col")
    z, core = me_col // CORES, me_col % CORES
    pos = snake(me_row, width)

    def ring_device(offset):
        return snake((pos + offset + row_dev) % row_dev, width)

    barrier = pltpu.get_barrier_semaphore()
    pl.semaphore_signal(barrier, inc=1, device_id={"col": z * CORES + 1 - core})
    peers = 1 + (z > 0).astype(jnp.int32) + (z < chips - 1).astype(jnp.int32)
    for offset in ((1, -1) if row_dev > 2 else (1,) * half):
        pl.semaphore_signal(barrier, inc=1, device_id={"row": ring_device(offset)})
        peers += 1

    @pl.when(z > 0)
    def _():
        pl.semaphore_signal(barrier, inc=1, device_id={"col": me_col - CORES})

    @pl.when(z < chips - 1)
    def _():
        pl.semaphore_signal(barrier, inc=1, device_id={"col": me_col + CORES})

    def load(q):
        spot = pl.ds(q * step_rows, step_rows)
        return pltpu.make_async_copy(v_ref.at[spot], loaded.at[spot], load_sem.at[q])

    for q in range(chunks):
        load(q).start()

    stored = tile_ref[...].astype(jnp.float32)
    kept = keep_ref[...].astype(jnp.float32)
    height = min(step_rows, TB)
    for lo in range(0, rows, height):
        if lo % step_rows == 0:
            load(lo // step_rows).wait()
        for b in range(cols // TB):
            r, c = slice(lo, lo + height), slice(b * TB, (b + 1) * TB)
            scale = jnp.broadcast_to(stored[b : b + 1, lo // TB : lo // TB + 1], (height, TB))
            tile = (loaded[r, c].astype(jnp.float32) * scale).astype(jnp.bfloat16)
            row_panel[me_col, r, c] = tile
            col_panel[pl.ds(pl.multiple_of(me_row * rows + lo, height), height), c] = tile

    pl.semaphore_wait(barrier, peers)

    def row_part(block, q):
        return row_panel.at[block, pl.ds(q * step_rows, step_rows)]

    def line_copy(zi, q, to_right):
        part = row_part(zi * CORES + core, q)
        return pltpu.make_async_remote_copy(
            src_ref=part, dst_ref=part,
            send_sem=line_send.at[to_right, zi, q], recv_sem=line_recv.at[zi, q],
            device_id={"col": me_col + (CORES if to_right else -CORES)},
        )

    def pair_copy(zi, q, lane):
        part = row_part(zi * CORES + lane, q)
        return pltpu.make_async_remote_copy(
            src_ref=part, dst_ref=part,
            send_sem=pair_send.at[zi, q], recv_sem=pair_recv.at[zi, q],
            device_id={"col": z * CORES + 1 - core},
        )

    def ring_copy(owner, q, to_right):
        start = pl.multiple_of(owner * rows + q * step_rows, step_rows)
        part = col_panel.at[pl.ds(start, step_rows)]
        return pltpu.make_async_remote_copy(
            src_ref=part, dst_ref=part,
            send_sem=ring_send.at[to_right, owner, q], recv_sem=ring_recv.at[owner, q],
            device_id={"row": ring_device(1 if to_right else -1)},
        )

    def on_ring(d, q, to_right):
        if d < half:
            return True
        return d == half and (q < chunks // 2) == bool(to_right)

    def relay(zi, q, to_right, wait):
        if wait:
            line_copy(zi, q, to_right).wait_recv()
        go = (z < chips - 1) if to_right else (z > 0)

        @pl.when(go)
        def _():
            line_copy(zi, q, to_right).start()

    for q in range(chunks):
        for to_right in (1, 0):
            relay(z, q, to_right, False)
            if on_ring(1, q, to_right):
                ring_copy(me_row, q, to_right).start()
        pair_copy(z, q, core).start()

    for to_right in (1, 0):
        first, end = (0, chips - 1) if to_right else (chips - 1, 0)

        @pl.when(z != first)
        def _():
            pl.semaphore_wait(token.at[to_right], 1)

        @pl.when(z != end)
        def _():
            pl.semaphore_signal(
                token.at[to_right], inc=1,
                device_id={"col": me_col + (CORES if to_right else -CORES)},
            )

    def line_step(t, q):
        for to_right in (1, 0):
            valid = (z >= t) if to_right else (z + t < chips)
            zi = z - t if to_right else z + t
            if t < chips:
                @pl.when(valid)
                def _():
                    relay(zi, q, to_right, True)
                    pair_copy(zi, q, core).start()

    def ring_step(t, q):
        for to_right in (1, 0):
            if on_ring(t, q, to_right):
                owner = ring_device(-t if to_right else t)
                ring_copy(owner, q, to_right).wait_recv()
                if on_ring(t + 1, q, to_right):
                    ring_copy(owner, q, to_right).start()

    def stat_copy(d):
        return pltpu.make_async_remote_copy(
            src_ref=stats.at[0], dst_ref=stats.at[d],
            send_sem=stat_send.at[d], recv_sem=stat_recv.at[d],
            device_id={"col": (me_col + d) % col_dev},
        )

    def send_stats():
        total = jnp.zeros((1, cols), jnp.float32)
        for i in range(row_dev):
            block = col_panel[i * rows : (i + 1) * rows].astype(jnp.float32)
            total += jnp.sum(block, axis=0, keepdims=True)
        stats[0] = total
        for d in range(1, col_dev):
            stat_copy(d).start()

    def product_sums():
        total = jnp.zeros((1, cols), jnp.float32)
        for d in range(col_dev):
            if d:
                stat_copy(d).wait()
            block = (me_col - d + col_dev) % col_dev
            inner = pl.ds(pl.multiple_of(block * cols, cols), cols)
            rest, terms = stats[d], []
            for _ in range(3):
                term = rest.astype(jnp.bfloat16).astype(jnp.float32)
                rest = rest - term
                terms.append(jnp.broadcast_to(term, (8, cols)))
            spread = jnp.dot(
                jnp.concatenate(terms, axis=0).astype(jnp.bfloat16), col_panel[inner],
                preferred_element_type=jnp.float32,
            )
            total += spread[16:17] + spread[8:9] + spread[0:1]
        return total

    def compute(zi, q, first=False):
        spot = pl.ds(pl.multiple_of(q * step_rows, step_rows), step_rows)
        total = None
        for lane in range(CORES):
            block = zi * CORES + lane
            inner = pl.ds(pl.multiple_of(block * cols, cols), cols)
            term = jnp.dot(
                row_panel[block, spot], col_panel[inner], preferred_element_type=jnp.float32
            )
            total = term if total is None else total + term
        if first:
            acc[spot] = total
        else:
            acc[spot] += total

    def take(zi, q, first=False):
        pair_copy(zi, q, 1 - core).wait_recv()
        compute(zi, q, first)

    def sides(t):
        return ((z >= t, z - t), (z + t < chips, z + t))

    def bulk(upto):
        @pl.loop(0, chunks)
        def _(q):
            take(z, q, True)
            for t in range(1, min(upto, chips - 1) + 1):
                for valid, zi in sides(t):
                    @pl.when(valid)
                    def _():
                        take(zi, q)

    def prune(q, cut):
        parts = []
        for b in range(cols // TB):
            c = slice(b * TB, (b + 1) * TB)
            part = jnp.zeros((1, TB), jnp.float32)
            for lo in range(q * step_rows, (q + 1) * step_rows, min(step_rows, TB)):
                r = slice(lo, lo + min(step_rows, TB))
                keep = jnp.broadcast_to(kept[b : b + 1, lo // TB : lo // TB + 1], (r.stop - lo, TB))
                pruned = jnp.maximum(acc[r, c] - cut[:, c], 0.0) * keep
                acc[r, c] = pruned
                part += jnp.sum(pruned, axis=0, keepdims=True)
            parts.append(part)
        return jnp.concatenate(parts, axis=1)

    def cuts():
        return 0.125 * thr_ref[...].astype(jnp.float32) * (product_sums() / order)

    part = jnp.zeros((1, cols), jnp.float32)
    last = max(chips - 1, half)
    if half == 0:
        send_stats()
        bulk(0)
    for t in range(1, last + 1):
        if t == half:
            for q in range(chunks):
                ring_step(t, q)
            send_stats()
            for q in range(chunks):
                line_step(t, q)
            bulk(t)
        else:
            if t == last and t > half:
                cut = cuts()
            for q in range(chunks):
                line_step(t, q)
                if t < half:
                    ring_step(t, q)
                else:
                    for valid, zi in sides(t):
                        @pl.when(valid)
                        def _():
                            take(zi, q)
                    if t == last:
                        part += prune(q, cut)
    if last <= half:
        cut = cuts()
        for q in range(chunks):
            part += prune(q, cut)

    sums[0] = part

    def sum_copy(d):
        return pltpu.make_async_remote_copy(
            src_ref=sums.at[0], dst_ref=sums.at[d],
            send_sem=sum_send.at[d], recv_sem=sum_recv.at[d],
            device_id={"row": (me_row + d) % row_dev},
        )

    for d in range(1, row_dev):
        sum_copy(d).start()
    for d in range(1, row_dev):
        sum_copy(d).wait()
        part += sums[d]
    totals_ref[...] = 1.0 / jnp.maximum(part / order, 0.1)

    for q in range(chunks):
        for zi in range(chips):
            pair_copy(zi, q, core).wait_send()

            @pl.when((z < chips - 1) & (z >= zi))
            def _():
                line_copy(zi, q, 1).wait_send()

            @pl.when((z > 0) & (z <= zi))
            def _():
                line_copy(zi, q, 0).wait_send()
        for d in range(0, half):
            for to_right in (1, 0):
                if on_ring(d + 1, q, to_right):
                    owner = ring_device(-d if to_right else d)
                    ring_copy(owner, q, to_right).wait_send()


def on_device(values, tile_mask, keep_mask, thr_index, *, row_dev, col_dev):
    rows, cols = values.shape
    width = max(w for w in range(1, row_dev + 1) if row_dev % w == 0 and w * w <= row_dev)
    chips = col_dev // CORES
    dma = pltpu.SemaphoreType.DMA
    vmem = pl.BlockSpec(memory_space=pltpu.VMEM)
    pruned, scale = pl.pallas_call(
        functools.partial(kernel, row_dev, col_dev, width, CHUNKS, rows * row_dev),
        out_shape=(
            pltpu.VMEM((rows, cols), jnp.float32),
            jax.ShapeDtypeStruct((1, cols), jnp.float32),
        ),
        in_specs=[pl.BlockSpec(memory_space=pl.ANY)] + [vmem] * 3,
        out_specs=(vmem, vmem),
        scratch_shapes=[
            pltpu.VMEM((col_dev, rows, cols), jnp.bfloat16),
            pltpu.VMEM((row_dev * rows, cols), jnp.bfloat16),
            pltpu.VMEM((row_dev, 1, cols), jnp.float32),
            pltpu.VMEM((col_dev, 1, cols), jnp.float32),
            dma((2, chips, CHUNKS)),
            dma((chips, CHUNKS)),
            dma((chips, CHUNKS)),
            dma((chips, CHUNKS)),
            dma((2, row_dev, CHUNKS)),
            dma((row_dev, CHUNKS)),
            dma((row_dev,)),
            dma((row_dev,)),
            dma((col_dev,)),
            dma((col_dev,)),
            pltpu.VMEM((rows, cols), jnp.bfloat16),
            dma((CHUNKS,)),
            pltpu.SemaphoreType.REGULAR((2,)),
        ],
        compiler_params=pltpu.CompilerParams(
            collective_id=0, has_side_effects=True,
            vmem_limit_bytes=63 * 2**20 - 4 * rows * cols + 2**19,
        ),
    )(values, tile_mask.T, keep_mask.T, thr_index.reshape(1, cols))
    return (pruned * scale).astype(jnp.bfloat16)


def solution(mesh):
    return jax.shard_map(
        functools.partial(on_device, row_dev=mesh.shape["row"], col_dev=mesh.shape["col"]),
        mesh=mesh,
        in_specs=(P("row", "col"), P("row", "col"), P("row", "col"), P("col")),
        out_specs=P("row", "col"),
        check_vma=False,
    )
```
